32 devices in a mesh: dp: 4 (over y, x), seq: 8 (over z, core).
Axes of the slice: x: 2, y: 2, z: 4, core: 2. Of those that a mesh axis runs over, the one named last changes fastest.
Arguments:
- queries: bfloat16 [16384, 128], P(('dp', 'seq')), parts along dimension 0, may hold values from -384 to 384
- users_of: int32 [16384], P(('dp', 'seq')), parts along dimension 0, may hold values from 0 to 3, as said below
- keys: bfloat16 [16, 8192, 128], P('dp', 'seq'), parts along dimension 0, may hold values from -12 to 12
- values: bfloat16 [16, 8192, 128], P('dp', 'seq'), parts along dimension 0, may hold values from -24 to 24
- lengths: int32 [16], P('dp'), parts along dimension 0, may hold values from 2 to 8192
Outputs:
- pooled: bfloat16 [16384, 128], P(('dp', 'seq')), parts along dimension 0
The draws below stay inside these ranges and needn't reach their ends.
There are 4 independent parts, one for each index of `dp`. The reference program is written for one: setup_inputs(seed, part) draws one part's arguments, and reference() takes and returns one part's arrays. A program takes and returns all parts, laid end to end along the dimension named above; each array names one. Nothing has to cross between parts.
Inputs may be any that keep to these rules, and one draw needn't show every extreme that they name: `users_of`: each candidate names one user of its group.
All inputs are finite; a program needn't handle non-finite values.
Results may differ from the reference program's by a relative error of at most 0.0065.
Values may be sent and summed in bfloat16 or wider, within the bound.
A program may use at most 192 MiB of HBM per device.

```python
import math
import jax
import jax.numpy as jnp
from jax import lax

D = 128
USERS = 4
CAND_DEV = 512
HIST = 8192
CANDS = 4096


def owner_draw(key):
    return jax.random.randint(jax.random.fold_in(key, 11), (CANDS,), 0, USERS, dtype=jnp.int32)


def key_field(key):
    field_rows = jax.random.normal(jax.random.fold_in(key, 23), (USERS, HIST, D), jnp.float32)
    field_rows = jnp.clip(field_rows, -6.0, 6.0)
    return field_rows


def draw_users_of(key, part):
    return owner_draw(key)


def draw_keys(key, part):
    return key_field(key).astype(jnp.bfloat16)


def draw_queries(key, part):
    drawn_rows = jnp.clip(2.0 * jax.random.normal(jax.random.fold_in(key, 31), (CANDS, D), jnp.float32), -12.0, 12.0)
    return drawn_rows.astype(jnp.bfloat16)


def with_ends(array, own_key, smallest, high):
    spot = [jax.random.randint(jax.random.fold_in(own_key, axis), (), 0, length) for axis, length in enumerate(array.shape)]
    longest = array.shape.index(max(array.shape))
    beside = spot[:longest] + [(spot[longest] + 1) % array.shape[longest]] + spot[longest + 1:]
    return array.at[tuple(spot)].set(smallest).at[tuple(beside)].set(high)


def level_of(stream_key, shape, split, smallest, high):
    def one(position, parts):
        heights = jax.random.uniform(jax.random.fold_in(jax.random.fold_in(stream_key, 6), position), (parts,), jnp.float32, smallest / len(split), high / len(split))
        return jnp.repeat(jnp.exp(heights), shape[position] // parts).reshape((-1,) + (1,) * (len(shape) - position - 1))

    factor_of = one(*split[0])
    for cut in split[1:]:
        factor_of = factor_of * one(*cut)
    return factor_of


def normal_values(rng, dims, scale, most, cuts=(), held_as=jnp.bfloat16):
    values = jax.random.normal(rng, dims, jnp.float32) * scale
    if len(cuts) > 0:
        values = level_of(rng, dims, cuts, -0.22, 0.18) * values
    return jnp.clip(values, min=-most, max=most).astype(held_as)


def setup_inputs(seed: int = 0, part: int = 0) -> dict:
    seeds = jax.random.split(jax.random.key(seed), 6)
    part_splits = jax.random.split(jax.random.fold_in(seeds[5], part), 6)
    queries = draw_queries(jax.random.fold_in(jax.random.fold_in(seeds[5], part), 71), part)
    users_of = draw_users_of(jax.random.fold_in(jax.random.fold_in(seeds[5], part), 71), part)
    keys = draw_keys(jax.random.fold_in(jax.random.fold_in(seeds[5], part), 71), part)
    values = normal_values(part_splits[3], (USERS, HIST, D), 4.0, 24.0, ((1, 8),))
    lengths = with_ends(jax.random.randint(part_splits[4], (USERS,), 2, HIST + 1), jax.random.fold_in(part_splits[4], 1), 2, HIST).astype(jnp.int32)
    return dict(queries=queries, users_of=users_of, keys=keys, values=values, lengths=lengths)


def reference(queries, users_of, keys, values, lengths):
    score_scale = 1.0 / math.sqrt(D)
    positions = jnp.arange(HIST, dtype=jnp.int32)

    def one_block(bundle):
        query_rows, owner_ids = bundle
        result = jnp.zeros((query_rows.shape[0], D), jnp.float32)
        for member in range(USERS):
            scores = jnp.dot(query_rows, keys[member].T, preferred_element_type=jnp.float32) * score_scale
            usable = (owner_ids[:, None] == member) & (positions[None, :] < lengths[member])
            scores = jnp.where(usable, scores, jnp.float32(-1e+30))
            row_max = lax.optimization_barrier(jnp.max(scores, axis=1, keepdims=True))
            weights = jnp.where(usable, jnp.exp(scores - row_max), jnp.float32(0.0))
            totals = lax.optimization_barrier(jnp.sum(weights, axis=1, keepdims=True))
            sums = jnp.dot(weights.astype(jnp.bfloat16), values[member], preferred_element_type=jnp.float32)
            mine = (owner_ids == member)[:, None]
            safe_totals = jnp.where(mine, totals, jnp.float32(1.0))
            result = jnp.where(mine, sums / safe_totals, result)
        return result.astype(jnp.bfloat16)
    blocks = CANDS // CAND_DEV
    query_blocks = queries.reshape(blocks, CAND_DEV, D)
    owner_blocks = users_of.reshape(blocks, CAND_DEV)
    return lax.map(one_block, (query_blocks, owner_blocks)).reshape(CANDS, D)
```

```python
import functools
import math

import jax
import jax.numpy as jnp
from jax import lax
from jax.experimental import pallas as pl
from jax.experimental.pallas import tpu as pltpu
from jax.sharding import PartitionSpec as P

CORES = 2
MESH = pl.DeviceIdType.MESH
LOW = -1e30


def turn(step, z, chips):
    inward = jnp.where(2 * z < chips, 1, -1)
    room = jnp.maximum(z, chips - 1 - z)
    return z + jnp.where(step < room, inward * (step + 1), -inward * (step - room + 1))


def kernel(
    chips, tile, coef,
    q_ref, u_ref, k_ref, v_ref, len_ref, o_ref,
    kp, vp, vt, qg, ug, pout, sout, pin, sin, own_p, own_s,
    kv_send, kv_recv, first_send, q_send, q_recv, u_send, u_recv, p_send, p_recv, s_send, s_recv,
):
    users, depth, width = k_ref.shape
    count = q_ref.shape[0]
    tiles = count // tile
    group = lax.axis_index("dp")
    me = lax.axis_index("seq")
    z = me // CORES
    core = me % CORES

    def at(chip, on=None):
        return (group, chip * CORES + (core if on is None else on))

    partner = at(z, 1 - core)

    barrier = pltpu.get_barrier_semaphore()
    pl.semaphore_signal(barrier, inc=1, device_id=partner, device_id_type=MESH)
    for nxt in (z + 1, z - 1):

        @pl.when((nxt >= 0) & (nxt < chips))
        def _(nxt=nxt):
            pl.semaphore_signal(barrier, inc=1, device_id=at(nxt), device_id_type=MESH)

    for user in range(users):
        vt[0, user * width:(user + 1) * width, :] = v_ref[user].T

    pl.semaphore_wait(barrier, 1 + jnp.where(z > 0, 1, 0) + jnp.where(z < chips - 1, 1, 0))

    def remote(src, dst, send, recv, to):
        return pltpu.make_async_remote_copy(
            src_ref=src, dst_ref=dst, send_sem=send, recv_sem=recv,
            device_id=to, device_id_type=MESH,
        )

    k_copy = remote(k_ref, kp, kv_send.at[0], kv_recv.at[0], partner)
    v_copy = remote(v_ref, vp, kv_send.at[1], kv_recv.at[1], partner)

    def relay(hop, part, act):
        for way in (1, -1):
            source = z - way * hop
            nxt = z + way

            @pl.when((source >= 0) & (source < chips))
            def _(way=way, source=source, nxt=nxt):
                if act == "pass":
                    take(source, part).wait_recv()
                    if part == 0:
                        take_u(source).wait_recv()

                @pl.when((nxt >= 0) & (nxt < chips))
                def _():
                    onward = [pass_q(source, part, nxt)]
                    if part == 0:
                        onward.append(pass_u(source, nxt))
                    for copy in onward:
                        if act == "pass":
                            copy.start()
                        else:
                            copy.wait_send()

    def take(source, part):
        rows = pl.ds(part * tile, tile)
        return remote(
            qg.at[source, rows], qg.at[source, rows], q_send.at[source, part], q_recv.at[source, part], partner
        )

    def take_u(source):
        return remote(ug.at[source], ug.at[source], u_send.at[source], u_recv.at[source], partner)

    def pass_q(source, part, to):
        rows = pl.ds(part * tile, tile)
        return remote(
            qg.at[source, rows], qg.at[source, rows], q_send.at[source, part], q_recv.at[source, part], at(to)
        )

    def pass_u(source, to):
        return remote(ug.at[source], ug.at[source], u_send.at[source], u_recv.at[source], at(to))

    def first(act):
        for side, way in enumerate((1, -1)):
            nxt = z + way

            @pl.when((nxt >= 0) & (nxt < chips))
            def _(side=side, nxt=nxt):
                copies = [
                    remote(u_ref, ug.at[z], first_send.at[side, tiles], u_recv.at[z], at(nxt))
                ]
                for part in range(tiles):
                    rows = pl.ds(part * tile, tile)
                    copies.append(
                        remote(
                            q_ref.at[rows], qg.at[z, rows], first_send.at[side, part],
                            q_recv.at[z, part], at(nxt),
                        )
                    )
                for copy in copies:
                    if act == "start":
                        copy.start()
                    else:
                        copy.wait_send()

    first("start")
    k_copy.start()
    v_copy.start()

    def queries(block, owners):
        turned = block.T
        return jnp.concatenate(
            [jnp.where(owners == user, turned, jnp.zeros_like(turned)) for user in range(users)], axis=0
        )

    place = lax.broadcasted_iota(jnp.int32, (depth, tile), 0)

    def score(turned, limit, key_ref):
        stacked = jnp.concatenate([key_ref[user] for user in range(users)], axis=1)
        scores = jnp.dot(stacked, turned, preferred_element_type=jnp.float32)
        scores = jnp.where(place < limit, scores, jnp.float32(LOW))
        return scores, jnp.max(scores, axis=0, keepdims=True)

    def blend(pair, which):
        scores, top = pair
        weights = jnp.exp2((scores - top) * coef)
        total = jnp.sum(weights, axis=0, keepdims=True)
        sums = jnp.dot(vt[which], weights.astype(jnp.bfloat16), preferred_element_type=jnp.float32)
        return top, total, sums

    def half(turned, limit, key_ref, which):
        return blend(score(turned, limit, key_ref), which)

    def limits(owners):
        length = jnp.zeros_like(owners)
        for user in range(users):
            length = jnp.where(owners == user, len_ref[user], length)
        return length - z * (CORES * depth)

    def pick(owners, value):
        picked = jnp.zeros((width, tile), jnp.float32)
        for user in range(users):
            picked = jnp.where(owners == user, value(slice(user * width, (user + 1) * width)), picked)
        return picked

    def merge(one, other):
        top = jnp.maximum(one[0], other[0])
        fa = jnp.exp2((one[0] - top) * coef)
        fb = jnp.exp2((other[0] - top) * coef)
        return top, one[1] * fa + other[1] * fb, fa, fb

    def near(turned, owners):
        return half(turned, limits(owners) - core * depth, k_ref, 0)

    def far(turned, owners):
        return half(turned, limits(owners) - (1 - core) * depth, kp, 1)

    def begin(block, owners):
        turned = queries(block, owners)
        lim = limits(owners)
        sa = score(turned, lim - core * depth, k_ref)
        sb = score(turned, lim - (1 - core) * depth, kp)
        return owners, sa, sb

    def finish(begun):
        owners, sa, sb = begun
        one = blend(sa, 0)
        other = blend(sb, 1)
        top, total, fa, fb = merge(one, other)
        return top, total, pick(owners, lambda rows: one[2][rows] * fa + other[2][rows] * fb)

    def cols(part):
        return slice(part * tile, (part + 1) * tile)

    for part in range(tiles):
        owners = u_ref[:, cols(part)]
        top, total, sums = near(queries(q_ref[cols(part), :], owners), owners)
        own_p[part] = pick(owners, lambda rows: sums[rows])
        own_s[0:1, cols(part)] = top
        own_s[1:2, cols(part)] = total

    for part in range(tiles):
        relay(1, part, "pass")

    k_copy.wait_recv()
    v_copy.wait_recv()
    for user in range(users):
        vt[1, user * width:(user + 1) * width, :] = vp[user].T

    def p_copy(step, part, slot, to):
        return remote(
            pout.at[step, part], pin.at[slot, part], p_send.at[step, part], p_recv.at[slot, part], at(to)
        )

    def s_copy(step, slot, to):
        return remote(sout.at[step], sin.at[slot], s_send.at[step], s_recv.at[slot], at(to))

    def serve(step, carry):
        chip = turn(step, z, chips)
        begun = [begin(qg[chip, cols(part), :], ug[chip, :, cols(part)]) for part in range(tiles)]
        for part in range(tiles):
            top, total, sums = finish(begun[part])
            pout[step, part] = sums.astype(jnp.bfloat16)
            sout[step, 0:1, cols(part)] = top
            sout[step, 1:2, cols(part)] = total
            p_copy(step, part, z, chip).start()
            relay(step + 2, part, "pass")
        s_copy(step, z, chip).start()
        return carry

    lax.fori_loop(0, chips - 1, serve, 0)

    for part in range(tiles):
        owners = u_ref[:, cols(part)]
        other = far(queries(q_ref[cols(part), :], owners), owners)
        top, total, fa, fb = merge((own_s[0:1, cols(part)], own_s[1:2, cols(part)]), other)
        own_p[part] = own_p[part] * fa + pick(owners, lambda rows: other[2][rows] * fb)
        own_s[0:1, cols(part)] = top
        own_s[1:2, cols(part)] = total

    for step in range(chips - 1):
        chip = turn(step, z, chips)
        s_copy(step, chip, chip).wait_recv()
        for part in range(tiles):
            p_copy(step, part, chip, chip).wait_recv()
            mine = own_s[0:1, cols(part)], own_s[1:2, cols(part)]
            theirs = sin[chip, 0:1, cols(part)], sin[chip, 1:2, cols(part)]
            top, total, fa, fb = merge(mine, theirs)
            sums = own_p[part] * fa + pin[chip, part].astype(jnp.float32) * fb
            if step < chips - 2:
                own_s[0:1, cols(part)] = top
                own_s[1:2, cols(part)] = total
                own_p[part] = sums
            else:
                o_ref[cols(part), :] = (sums / total).T.astype(o_ref.dtype)

    k_copy.wait_send()
    v_copy.wait_send()
    first("end")
    for hop in range(1, chips - 1):
        for part in range(tiles):
            relay(hop, part, "end")
    for step in range(chips - 1):
        chip = turn(step, z, chips)
        for part in range(tiles):
            p_copy(step, part, z, chip).wait_send()
        s_copy(step, z, chip).wait_send()


def local(size, queries, users_of, keys, values, lengths):
    chips = size // CORES
    count, width = queries.shape
    users, depth, _ = keys.shape
    tile = min(256, count)
    tiles = count // tile
    coef = math.log2(math.e) / math.sqrt(width)
    dma = pltpu.SemaphoreType.DMA
    vmem = pl.BlockSpec(memory_space=pltpu.VMEM)
    return pl.pallas_call(
        functools.partial(kernel, chips, tile, coef),
        out_shape=pltpu.VMEM((count, width), jnp.bfloat16),
        in_specs=[vmem] * 4 + [pl.BlockSpec(memory_space=pltpu.SMEM)],
        out_specs=vmem,
        scratch_shapes=[
            pltpu.VMEM(keys.shape, jnp.bfloat16),
            pltpu.VMEM(values.shape, jnp.bfloat16),
            pltpu.VMEM((2, users * width, depth), jnp.bfloat16),
            pltpu.VMEM((chips, count, width), jnp.bfloat16),
            pltpu.VMEM((chips, 1, count), jnp.int32),
            pltpu.VMEM((chips - 1, tiles, width, tile), jnp.bfloat16),
            pltpu.VMEM((chips - 1, 2, count), jnp.float32),
            pltpu.VMEM((chips, tiles, width, tile), jnp.bfloat16),
            pltpu.VMEM((chips, 2, count), jnp.float32),
            pltpu.VMEM((tiles, width, tile), jnp.float32),
            pltpu.VMEM((2, count), jnp.float32),
            dma((2,)), dma((2,)),
            dma((2, tiles + 1)), dma((chips, tiles)), dma((chips, tiles)),
            dma((chips,)), dma((chips,)),
            dma((chips - 1, tiles)), dma((chips, tiles)),
            dma((chips - 1,)), dma((chips,)),
        ],
        compiler_params=pltpu.CompilerParams(
            collective_id=0, has_side_effects=True, vmem_limit_bytes=56 * 1024 * 1024
        ),
    )(queries, users_of.reshape(1, count), keys, values, lengths)


def solution(mesh):
    return jax.shard_map(
        functools.partial(local, mesh.shape["seq"]),
        mesh=mesh,
        in_specs=(
            P(("dp", "seq"), None),
            P(("dp", "seq")),
            P("dp", "seq", None),
            P("dp", "seq", None),
            P("dp"),
        ),
        out_specs=P(("dp", "seq"), None),
        check_vma=False,
    )
```

```python
import functools
import math

import jax
import jax.numpy as jnp
from jax import lax
from jax.experimental import pallas as pl
from jax.experimental.pallas import tpu as pltpu
from jax.sharding import PartitionSpec as P

CORES = 2
MESH = pl.DeviceIdType.MESH
LOW = -1e30


def turn(step, z, chips):
    up = step - z
    other = jnp.bitwise_xor(jnp.maximum(up, 0), 1)
    up = jnp.where((z > 0) & (z + other + 1 < chips), other, up)
    return jnp.where(step < z, z - 1 - step, z + 1 + up)


def kernel(
    chips, tile, coef,
    q_hbm, u_hbm, k_hbm, v_hbm, len_ref, o_ref,
    q_ref, u_ref, k_ref, v_ref, kp, vp, vt, qg, ug, pout, sout, pin, sin, own_p, own_s,
    load, ready, kv_send, kv_recv, first_send, q_send, q_recv, u_send, u_recv, p_send, p_recv, s_send, s_recv,
):
    users, depth, width = k_ref.shape
    count = q_ref.shape[0]
    tiles = count // tile
    group = lax.axis_index("dp")
    me = lax.axis_index("seq")
    z = me // CORES
    core = me % CORES

    def at(chip, on=None):
        return (group, chip * CORES + (core if on is None else on))

    partner = at(z, 1 - core)

    loads = [
        pltpu.make_async_copy(src, dst, load.at[n])
        for n, (src, dst) in enumerate(((u_hbm, u_ref), (q_hbm, q_ref), (k_hbm, k_ref), (v_hbm, v_ref)))
    ]
    for copy in loads:
        copy.start()

    barrier = pltpu.get_barrier_semaphore()
    pl.semaphore_signal(barrier, inc=1, device_id=partner, device_id_type=MESH)
    pl.semaphore_wait(barrier, 1 + jnp.where(z > 0, 1, 0))

    @pl.when(z < chips - 1)
    def _():
        pl.semaphore_signal(barrier, inc=1, device_id=at(z + 1), device_id_type=MESH)

    @pl.when(z > 0)
    def _():
        pl.semaphore_signal(ready, inc=1, device_id=at(z - 1), device_id_type=MESH)

    def remote(src, dst, send, recv, to):
        return pltpu.make_async_remote_copy(
            src_ref=src, dst_ref=dst, send_sem=send, recv_sem=recv,
            device_id=to, device_id_type=MESH,
        )

    k_copy = remote(k_ref, kp, kv_send.at[0], kv_recv.at[0], partner)
    v_copy = remote(v_ref, vp, kv_send.at[1], kv_recv.at[1], partner)

    def relay(hop, part, act):
        for way in (1, -1):
            source = z - way * hop
            nxt = z + way

            @pl.when((source >= 0) & (source < chips))
            def _(way=way, source=source, nxt=nxt):
                if act == "pass":
                    take(source, part).wait_recv()
                    if part == 0:
                        take_u(source).wait_recv()

                @pl.when((nxt >= 0) & (nxt < chips))
                def _():
                    onward = [pass_q(source, part, nxt)]
                    if part == 0:
                        onward.append(pass_u(source, nxt))
                    for copy in onward:
                        if act == "pass":
                            copy.start()
                        else:
                            copy.wait_send()

    def take(source, part):
        rows = pl.ds(part * tile, tile)
        return remote(
            qg.at[source, rows], qg.at[source, rows], q_send.at[source, part], q_recv.at[source, part], partner
        )

    def take_u(source):
        return remote(ug.at[source], ug.at[source], u_send.at[source], u_recv.at[source], partner)

    def pass_q(source, part, to):
        rows = pl.ds(part * tile, tile)
        return remote(
            qg.at[source, rows], qg.at[source, rows], q_send.at[source, part], q_recv.at[source, part], at(to)
        )

    def pass_u(source, to):
        return remote(ug.at[source], ug.at[source], u_send.at[source], u_recv.at[source], at(to))

    def first(side, act):
        nxt = z + (1, -1)[side]

        @pl.when((nxt >= 0) & (nxt < chips))
        def _():
            if act == "start" and side == 0:
                pl.semaphore_wait(ready, 1)
            copies = [remote(u_ref, ug.at[z], first_send.at[side, tiles], u_recv.at[z], at(nxt))]
            for part in range(tiles):
                rows = pl.ds(part * tile, tile)
                copies.append(
                    remote(
                        q_ref.at[rows], qg.at[z, rows], first_send.at[side, part],
                        q_recv.at[z, part], at(nxt),
                    )
                )
            for copy in copies:
                if act == "start":
                    copy.start()
                else:
                    copy.wait_send()

    loads[0].wait()
    loads[1].wait()
    first(1, "start")
    loads[2].wait()
    k_copy.start()
    loads[3].wait()
    v_copy.start()
    first(0, "start")

    for user in range(users):
        vt[0, user * width:(user + 1) * width, :] = v_ref[user].T

    def queries(block, owners):
        turned = block.T
        return jnp.concatenate(
            [jnp.where(owners == user, turned, jnp.zeros_like(turned)) for user in range(users)], axis=0
        )

    place = lax.broadcasted_iota(jnp.int32, (depth, tile), 0)

    def score(turned, limit, key_ref):
        stacked = jnp.concatenate([key_ref[user] for user in range(users)], axis=1)
        scores = jnp.dot(stacked, turned, preferred_element_type=jnp.float32)
        scores = jnp.where(place < limit, scores, jnp.float32(LOW))
        return scores, jnp.max(scores, axis=0, keepdims=True)

    def blend(pair, which):
        scores, top = pair
        weights = jnp.exp2((scores - top) * coef)
        total = jnp.sum(weights, axis=0, keepdims=True)
        sums = jnp.dot(vt[which], weights.astype(jnp.bfloat16), preferred_element_type=jnp.float32)
        return top, total, sums

    def half(turned, limit, key_ref, which):
        return blend(score(turned, limit, key_ref), which)

    def limits(owners):
        length = jnp.zeros_like(owners)
        for user in range(users):
            length = jnp.where(owners == user, len_ref[user], length)
        return length - z * (CORES * depth)

    def pick(owners, value):
        picked = jnp.zeros((width, tile), jnp.float32)
        for user in range(users):
            picked = jnp.where(owners == user, value(slice(user * width, (user + 1) * width)), picked)
        return picked

    def merge(one, other):
        top = jnp.maximum(one[0], other[0])
        fa = jnp.exp2((one[0] - top) * coef)
        fb = jnp.exp2((other[0] - top) * coef)
        return top, one[1] * fa + other[1] * fb, fa, fb

    def near(turned, owners):
        return half(turned, limits(owners) - core * depth, k_ref, 0)

    def far(turned, owners):
        return half(turned, limits(owners) - (1 - core) * depth, kp, 1)

    def begin(block, owners):
        turned = queries(block, owners)
        lim = limits(owners)
        sa = score(turned, lim - core * depth, k_ref)
        sb = score(turned, lim - (1 - core) * depth, kp)
        return owners, sa, sb

    def finish(begun):
        owners, sa, sb = begun
        one = blend(sa, 0)
        other = blend(sb, 1)
        top, total, fa, fb = merge(one, other)
        return top, total, pick(owners, lambda rows: one[2][rows] * fa + other[2][rows] * fb)

    def cols(part):
        return slice(part * tile, (part + 1) * tile)

    for part in range(tiles):
        owners = u_ref[:, cols(part)]
        top, total, sums = near(queries(q_ref[cols(part), :], owners), owners)
        own_p[part] = pick(owners, lambda rows: sums[rows])
        own_s[0:1, cols(part)] = top
        own_s[1:2, cols(part)] = total

    for part in range(tiles):
        relay(1, part, "pass")

    k_copy.wait_recv()
    v_copy.wait_recv()
    for user in range(users):
        vt[1, user * width:(user + 1) * width, :] = vp[user].T

    def p_copy(step, part, slot, to):
        return remote(
            pout.at[step, part], pin.at[slot, part], p_send.at[step, part], p_recv.at[slot, part], at(to)
        )

    def s_copy(step, slot, to):
        return remote(sout.at[step], sin.at[slot], s_send.at[step], s_recv.at[slot], at(to))

    def serve(step, carry):
        chip = turn(step, z, chips)
        begun = [begin(qg[chip, cols(part), :], ug[chip, :, cols(part)]) for part in range(tiles)]
        for part in range(tiles):
            top, total, sums = finish(begun[part])
            pout[step, part] = sums.astype(jnp.bfloat16)
            sout[step, 0:1, cols(part)] = top
            sout[step, 1:2, cols(part)] = total
            p_copy(step, part, z, chip).start()
            relay(step + 2, part, "pass")
        s_copy(step, z, chip).start()
        return carry

    def own_far():
        for part in range(tiles):
            owners = u_ref[:, cols(part)]
            other = far(queries(q_ref[cols(part), :], owners), owners)
            top, total, fa, fb = merge((own_s[0:1, cols(part)], own_s[1:2, cols(part)]), other)
            own_p[part] = own_p[part] * fa + pick(owners, lambda rows: other[2][rows] * fb)
            own_s[0:1, cols(part)] = top
            own_s[1:2, cols(part)] = total

    @pl.when(z == 0)
    def _():
        own_far()

    lax.fori_loop(0, chips - 1, serve, 0)

    @pl.when(z > 0)
    def _():
        own_far()

    for step in range(chips - 1):
        chip = turn(step, z, chips)
        s_copy(step, chip, chip).wait_recv()
        for part in range(tiles):
            p_copy(step, part, chip, chip).wait_recv()
            mine = own_s[0:1, cols(part)], own_s[1:2, cols(part)]
            theirs = sin[chip, 0:1, cols(part)], sin[chip, 1:2, cols(part)]
            top, total, fa, fb = merge(mine, theirs)
            sums = own_p[part] * fa + pin[chip, part].astype(jnp.float32) * fb
            if step < chips - 2:
                own_s[0:1, cols(part)] = top
                own_s[1:2, cols(part)] = total
                own_p[part] = sums
            else:
                o_ref[cols(part), :] = (sums / total).T.astype(o_ref.dtype)

    k_copy.wait_send()
    v_copy.wait_send()
    first(0, "end")
    first(1, "end")
    for hop in range(1, chips - 1):
        for part in range(tiles):
            relay(hop, part, "end")
    for step in range(chips - 1):
        chip = turn(step, z, chips)
        for part in range(tiles):
            p_copy(step, part, z, chip).wait_send()
        s_copy(step, z, chip).wait_send()


def local(size, queries, users_of, keys, values, lengths):
    chips = size // CORES
    count, width = queries.shape
    users, depth, _ = keys.shape
    tile = min(256, count)
    tiles = count // tile
    coef = math.log2(math.e) / math.sqrt(width)
    dma = pltpu.SemaphoreType.DMA
    vmem = pl.BlockSpec(memory_space=pltpu.VMEM)
    return pl.pallas_call(
        functools.partial(kernel, chips, tile, coef),
        out_shape=pltpu.VMEM((count, width), jnp.bfloat16),
        in_specs=[pl.BlockSpec(memory_space=pl.ANY)] * 4 + [pl.BlockSpec(memory_space=pltpu.SMEM)],
        out_specs=vmem,
        scratch_shapes=[
            pltpu.VMEM((count, width), jnp.bfloat16),
            pltpu.VMEM((1, count), jnp.int32),
            pltpu.VMEM(keys.shape, jnp.bfloat16),
            pltpu.VMEM(values.shape, jnp.bfloat16),
            pltpu.VMEM(keys.shape, jnp.bfloat16),
            pltpu.VMEM(values.shape, jnp.bfloat16),
            pltpu.VMEM((2, users * width, depth), jnp.bfloat16),
            pltpu.VMEM((chips, count, width), jnp.bfloat16),
            pltpu.VMEM((chips, 1, count), jnp.int32),
            pltpu.VMEM((chips - 1, tiles, width, tile), jnp.bfloat16),
            pltpu.VMEM((chips - 1, 2, count), jnp.float32),
            pltpu.VMEM((chips, tiles, width, tile), jnp.bfloat16),
            pltpu.VMEM((chips, 2, count), jnp.float32),
            pltpu.VMEM((tiles, width, tile), jnp.float32),
            pltpu.VMEM((2, count), jnp.float32),
            dma((4,)), pltpu.SemaphoreType.REGULAR, dma((2,)), dma((2,)),
            dma((2, tiles + 1)), dma((chips, tiles)), dma((chips, tiles)),
            dma((chips,)), dma((chips,)),
            dma((chips - 1, tiles)), dma((chips, tiles)),
            dma((chips - 1,)), dma((chips,)),
        ],
        compiler_params=pltpu.CompilerParams(
            collective_id=0, has_side_effects=True, vmem_limit_bytes=56 * 1024 * 1024
        ),
    )(queries, users_of.reshape(1, count), keys, values, lengths)


def solution(mesh):
    return jax.shard_map(
        functools.partial(local, mesh.shape["seq"]),
        mesh=mesh,
        in_specs=(
            P(("dp", "seq"), None),
            P(("dp", "seq")),
            P("dp", "seq", None),
            P("dp", "seq", None),
            P("dp"),
        ),
        out_specs=P(("dp", "seq"), None),
        check_vma=False,
    )
```

```python
import functools
import math

import jax
import jax.numpy as jnp
from jax import lax
from jax.experimental import pallas as pl
from jax.experimental.pallas import tpu as pltpu
from jax.sharding import PartitionSpec as P

CORES = 2
MESH = pl.DeviceIdType.MESH
LOW = -1e30


def turn(step, z, chips):
    up = step - z
    other = jnp.bitwise_xor(jnp.maximum(up, 0), 1)
    up = jnp.where((z > 0) & (z + other + 1 < chips), other, up)
    return jnp.where(step < z, z - 1 - step, z + 1 + up)


def kernel(
    chips, tile, coef,
    q_hbm, u_hbm, k_hbm, v_hbm, len_ref, o_ref,
    q_ref, u_ref, k_ref, v_ref, kp, vp, vt, qg, ug, pout, sout, pin, sin, own_p, own_s,
    load, ready, kv_send, kv_recv, first_send, q_send, q_recv, u_send, u_recv, p_send, p_recv, s_send, s_recv,
):
    users, depth, width = k_ref.shape
    count = q_ref.shape[0]
    tiles = count // tile
    group = lax.axis_index("dp")
    me = lax.axis_index("seq")
    z = me // CORES
    core = me % CORES

    def at(chip, on=None):
        return (group, chip * CORES + (core if on is None else on))

    partner = at(z, 1 - core)

    loads = [
        pltpu.make_async_copy(src, dst, load.at[n])
        for n, (src, dst) in enumerate(((u_hbm, u_ref), (q_hbm, q_ref), (k_hbm, k_ref), (v_hbm, v_ref)))
    ]
    for copy in loads:
        copy.start()

    barrier = pltpu.get_barrier_semaphore()
    pl.semaphore_signal(barrier, inc=1, device_id=partner, device_id_type=MESH)
    pl.semaphore_wait(barrier, 1 + jnp.where(z > 0, 1, 0))

    @pl.when(z < chips - 1)
    def _():
        pl.semaphore_signal(barrier, inc=1, device_id=at(z + 1), device_id_type=MESH)

    @pl.when(z > 0)
    def _():
        pl.semaphore_signal(ready, inc=1, device_id=at(z - 1), device_id_type=MESH)

    def remote(src, dst, send, recv, to):
        return pltpu.make_async_remote_copy(
            src_ref=src, dst_ref=dst, send_sem=send, recv_sem=recv,
            device_id=to, device_id_type=MESH,
        )

    k_copy = remote(k_ref, kp, kv_send.at[0], kv_recv.at[0], partner)
    v_copy = remote(v_ref, vp, kv_send.at[1], kv_recv.at[1], partner)

    def relay(hop, part, way, act):
        source = z - way * hop
        nxt = z + way

        @pl.when((source >= 0) & (source < chips) & (nxt >= 0) & (nxt < chips))
        def _():
            onward = [pass_q(source, part, nxt)]
            if part == 0:
                onward.append(pass_u(source, nxt))
            for copy in onward:
                if act == "pass":
                    copy.wait_recv()
                    copy.start()
                else:
                    copy.wait_send()

    def arrived(source, part):
        @pl.when(jnp.where(source < z, z == chips - 1, z == 0))
        def _():
            take(source, part).wait_recv()
            if part == 0:
                take_u(source).wait_recv()

    def take(source, part):
        rows = pl.ds(part * tile, tile)
        return remote(
            qg.at[source, rows], qg.at[source, rows], q_send.at[source, part], q_recv.at[source, part], partner
        )

    def take_u(source):
        return remote(ug.at[source], ug.at[source], u_send.at[source], u_recv.at[source], partner)

    def pass_q(source, part, to):
        rows = pl.ds(part * tile, tile)
        return remote(
            qg.at[source, rows], qg.at[source, rows], q_send.at[source, part], q_recv.at[source, part], at(to)
        )

    def pass_u(source, to):
        return remote(ug.at[source], ug.at[source], u_send.at[source], u_recv.at[source], at(to))

    def first(side, act):
        nxt = z + (1, -1)[side]

        @pl.when((nxt >= 0) & (nxt < chips))
        def _():
            if act == "start" and side == 0:
                pl.semaphore_wait(ready, 1)
            copies = [remote(u_ref, ug.at[z], first_send.at[side, tiles], u_recv.at[z], at(nxt))]
            for part in range(tiles):
                rows = pl.ds(part * tile, tile)
                copies.append(
                    remote(
                        q_ref.at[rows], qg.at[z, rows], first_send.at[side, part],
                        q_recv.at[z, part], at(nxt),
                    )
                )
            for copy in copies:
                if act == "start":
                    copy.start()
                else:
                    copy.wait_send()

    loads[0].wait()
    loads[1].wait()
    first(1, "start")
    loads[2].wait()
    k_copy.start()
    loads[3].wait()
    v_copy.start()
    first(0, "start")

    for user in range(users):
        vt[0, user * width:(user + 1) * width, :] = v_ref[user].T

    def queries(block, owners):
        turned = block.T
        return jnp.concatenate(
            [jnp.where(owners == user, turned, jnp.zeros_like(turned)) for user in range(users)], axis=0
        )

    place = lax.broadcasted_iota(jnp.int32, (depth, tile), 0)

    def score(turned, limit, key_ref):
        stacked = jnp.concatenate([key_ref[user] for user in range(users)], axis=1)
        scores = jnp.dot(stacked, turned, preferred_element_type=jnp.float32)
        scores = jnp.where(place < limit, scores, jnp.float32(LOW))
        return scores, jnp.max(scores, axis=0, keepdims=True)

    def blend(pair, which):
        scores, top = pair
        weights = jnp.exp2((scores - top) * coef)
        total = jnp.sum(weights, axis=0, keepdims=True)
        sums = jnp.dot(vt[which], weights.astype(jnp.bfloat16), preferred_element_type=jnp.float32)
        return top, total, sums

    def half(turned, limit, key_ref, which):
        return blend(score(turned, limit, key_ref), which)

    def limits(owners):
        length = jnp.zeros_like(owners)
        for user in range(users):
            length = jnp.where(owners == user, len_ref[user], length)
        return length - z * (CORES * depth)

    def pick(owners, value):
        picked = jnp.zeros((width, tile), jnp.float32)
        for user in range(users):
            picked = jnp.where(owners == user, value(slice(user * width, (user + 1) * width)), picked)
        return picked

    def merge(one, other):
        top = jnp.maximum(one[0], other[0])
        fa = jnp.exp2((one[0] - top) * coef)
        fb = jnp.exp2((other[0] - top) * coef)
        return top, one[1] * fa + other[1] * fb, fa, fb

    def near(turned, owners):
        return half(turned, limits(owners) - core * depth, k_ref, 0)

    def far(turned, owners):
        return half(turned, limits(owners) - (1 - core) * depth, kp, 1)

    def begin(block, owners):
        turned = queries(block, owners)
        lim = limits(owners)
        sa = score(turned, lim - core * depth, k_ref)
        sb = score(turned, lim - (1 - core) * depth, kp)
        return owners, sa, sb

    def finish(begun):
        owners, sa, sb = begun
        one = blend(sa, 0)
        other = blend(sb, 1)
        top, total, fa, fb = merge(one, other)
        return top, total, pick(owners, lambda rows: one[2][rows] * fa + other[2][rows] * fb)

    def cols(part):
        return slice(part * tile, (part + 1) * tile)

    for part in range(tiles):
        owners = u_ref[:, cols(part)]
        top, total, sums = near(queries(q_ref[cols(part), :], owners), owners)
        own_p[part] = pick(owners, lambda rows: sums[rows])
        own_s[0:1, cols(part)] = top
        own_s[1:2, cols(part)] = total

    for part in range(tiles):
        relay(1, part, 1, "pass")
        relay(1, part, -1, "pass")

    k_copy.wait_recv()
    v_copy.wait_recv()
    for user in range(users):
        vt[1, user * width:(user + 1) * width, :] = vp[user].T

    def p_copy(step, part, slot, to):
        return remote(
            pout.at[step, part], pin.at[slot, part], p_send.at[step, part], p_recv.at[slot, part], at(to)
        )

    def s_copy(step, slot, to):
        return remote(sout.at[step], sin.at[slot], s_send.at[step], s_recv.at[slot], at(to))

    def serve(step, carry):
        chip = turn(step, z, chips)
        for part in range(tiles):
            arrived(chip, part)
        begun = [begin(qg[chip, cols(part), :], ug[chip, :, cols(part)]) for part in range(tiles)]
        for part in range(tiles):
            top, total, sums = finish(begun[part])
            pout[step, part] = sums.astype(jnp.bfloat16)
            sout[step, 0:1, cols(part)] = top
            sout[step, 1:2, cols(part)] = total
            p_copy(step, part, z, chip).start()
        for part in range(tiles):
            relay(step + 2, part, 1, "pass")
            relay(step + 2, part, -1, "pass")
        s_copy(step, z, chip).start()
        return carry

    def own_far():
        for part in range(tiles):
            owners = u_ref[:, cols(part)]
            other = far(queries(q_ref[cols(part), :], owners), owners)
            top, total, fa, fb = merge((own_s[0:1, cols(part)], own_s[1:2, cols(part)]), other)
            own_p[part] = own_p[part] * fa + pick(owners, lambda rows: other[2][rows] * fb)
            own_s[0:1, cols(part)] = top
            own_s[1:2, cols(part)] = total

    @pl.when(z == 0)
    def _():
        own_far()

    lax.fori_loop(0, chips - 1, serve, 0)

    @pl.when(z > 0)
    def _():
        own_far()

    for step in range(chips - 1):
        chip = turn(step, z, chips)
        s_copy(step, chip, chip).wait_recv()
        for part in range(tiles):
            p_copy(step, part, chip, chip).wait_recv()
            mine = own_s[0:1, cols(part)], own_s[1:2, cols(part)]
            theirs = sin[chip, 0:1, cols(part)], sin[chip, 1:2, cols(part)]
            top, total, fa, fb = merge(mine, theirs)
            sums = own_p[part] * fa + pin[chip, part].astype(jnp.float32) * fb
            if step < chips - 2:
                own_s[0:1, cols(part)] = top
                own_s[1:2, cols(part)] = total
                own_p[part] = sums
            else:
                o_ref[cols(part), :] = (sums / total).T.astype(o_ref.dtype)

    k_copy.wait_send()
    v_copy.wait_send()
    first(0, "end")
    first(1, "end")
    for hop in range(1, chips - 1):
        for part in range(tiles):
            relay(hop, part, 1, "end")
            relay(hop, part, -1, "end")
    for step in range(chips - 1):
        chip = turn(step, z, chips)
        for part in range(tiles):
            p_copy(step, part, z, chip).wait_send()
        s_copy(step, z, chip).wait_send()


def local(size, queries, users_of, keys, values, lengths):
    chips = size // CORES
    count, width = queries.shape
    users, depth, _ = keys.shape
    tile = min(256, count)
    tiles = count // tile
    coef = math.log2(math.e) / math.sqrt(width)
    dma = pltpu.SemaphoreType.DMA
    vmem = pl.BlockSpec(memory_space=pltpu.VMEM)
    return pl.pallas_call(
        functools.partial(kernel, chips, tile, coef),
        out_shape=pltpu.VMEM((count, width), jnp.bfloat16),
        in_specs=[pl.BlockSpec(memory_space=pl.ANY)] * 4 + [pl.BlockSpec(memory_space=pltpu.SMEM)],
        out_specs=vmem,
        scratch_shapes=[
            pltpu.VMEM((count, width), jnp.bfloat16),
            pltpu.VMEM((1, count), jnp.int32),
            pltpu.VMEM(keys.shape, jnp.bfloat16),
            pltpu.VMEM(values.shape, jnp.bfloat16),
            pltpu.VMEM(keys.shape, jnp.bfloat16),
            pltpu.VMEM(values.shape, jnp.bfloat16),
            pltpu.VMEM((2, users * width, depth), jnp.bfloat16),
            pltpu.VMEM((chips, count, width), jnp.bfloat16),
            pltpu.VMEM((chips, 1, count), jnp.int32),
            pltpu.VMEM((chips - 1, tiles, width, tile), jnp.bfloat16),
            pltpu.VMEM((chips - 1, 2, count), jnp.float32),
            pltpu.VMEM((chips, tiles, width, tile), jnp.bfloat16),
            pltpu.VMEM((chips, 2, count), jnp.float32),
            pltpu.VMEM((tiles, width, tile), jnp.float32),
            pltpu.VMEM((2, count), jnp.float32),
            dma((4,)), pltpu.SemaphoreType.REGULAR, dma((2,)), dma((2,)),
            dma((2, tiles + 1)), dma((chips, tiles)), dma((chips, tiles)),
            dma((chips,)), dma((chips,)),
            dma((chips - 1, tiles)), dma((chips, tiles)),
            dma((chips - 1,)), dma((chips,)),
        ],
        compiler_params=pltpu.CompilerParams(
            collective_id=0, has_side_effects=True, vmem_limit_bytes=56 * 1024 * 1024
        ),
    )(queries, users_of.reshape(1, count), keys, values, lengths)


def solution(mesh):
    return jax.shard_map(
        functools.partial(local, mesh.shape["seq"]),
        mesh=mesh,
        in_specs=(
            P(("dp", "seq"), None),
            P(("dp", "seq")),
            P("dp", "seq", None),
            P("dp", "seq", None),
            P("dp"),
        ),
        out_specs=P(("dp", "seq"), None),
        check_vma=False,
    )
```
